512 devices in a mesh: section: 4 (over x), expert: 32 (over z, core), dp: 4 (over y).
Axes of the slice: x: 4, y: 4, z: 16, core: 2. Of those that a mesh axis runs over, the one named last changes fastest.
Arguments:
- fwd_input: bfloat16 [4, 256, 2048], P('section', 'dp', 'expert'), may hold values from -6 to 6
- fresh_input: bfloat16 [1, 256, 2048], P(None, 'dp', 'expert'), may hold values from -6 to 6
- fwd_experts: int32 [4, 2, 256, 2], P('section', None, 'dp'), may hold values from 0 to 3, all different within a row; in each aligned block of 64 rows (0 to 63, 64 to 127, ..., all dimensions but the last counted through in order) at most 36 rows name the same one
- fwd_gates: float32 [4, 2, 256, 2], P('section', None, 'dp'), may hold values from 0.2 to 1
- bwd_saved: bfloat16 [4, 2, 256, 2048], P('section', None, 'dp', 'expert'), may hold values from -6 to 6
- bwd_experts: int32 [4, 2, 256, 2], P('section', None, 'dp'), may hold values from 0 to 3, all different within a row; in each aligned block of 64 rows (0 to 63, 64 to 127, ..., all dimensions but the last counted through in order) at most 36 rows name the same one
- bwd_gates: float32 [4, 2, 256, 2], P('section', None, 'dp'), may hold values from 0.2 to 1
- out_grad: bfloat16 [4, 256, 2048], P('section', 'dp', 'expert'), may hold values from -6 to 6
- fresh_grad: bfloat16 [1, 256, 2048], P(None, 'dp', 'expert'), may hold values from -6 to 6
- gate_proj: bfloat16 [4, 4, 7168, 2048], P('section', 'dp', 'expert'), may hold values from -0.125 to 0.125
- down_proj: bfloat16 [4, 4, 7168, 2048], P('section', 'dp', 'expert'), may hold values from -0.0625 to 0.0625
Outputs:
- fwd_output: bfloat16 [4, 2, 256, 2048], P('section', None, 'dp', 'expert')
- input_grad: bfloat16 [4, 2, 256, 2048], P('section', None, 'dp', 'expert')
- gate_grad: bfloat16 [4, 4, 7168, 2048], P('section', 'dp', 'expert')
- down_grad: bfloat16 [4, 4, 7168, 2048], P('section', 'dp', 'expert')
The draws below stay inside these ranges and needn't reach their ends.
Inputs may be any that keep to these rules, and one draw needn't show every extreme that they name: `fwd_experts`: each token names two different experts. In every aligned block of 64 tokens (one index of dp, one section and step) no expert is named more than 36 times, and in some blocks one expert is named exactly 36 times. `bwd_experts`: each token names two different experts. In every aligned block of 64 tokens (one index of dp, one section and step) no expert is named more than 36 times, and in some blocks one expert is named exactly 36 times.
All inputs are finite; a program needn't handle non-finite values.
Results may differ from the reference program's by a relative error of at most 0.0062.
Values may be sent and summed in bfloat16 or wider, within the bound.
No kernel may reach another device: no remote copies, remote signals or barrier semaphores. Data moves between devices by JAX's collectives and lax.ppermute only.
A program may use at most 64 MiB of HBM per device.

```python
import math
import jax
import jax.numpy as jnp
import numpy as np
from jax import lax

D = 2048
FF = 7168
EXPERTS = 4
TOK_DEV = 64
TICKS = 2
CAP = 36
SECTIONS = 4
BLOCKS = 32
TOKENS = 256


def block_scale(own_key, dims, shards, smallest, high):
    gain, own = 1.0, jax.random.fold_in(own_key, 6)
    for dim, shards_of in shards:
        steps = jnp.exp(jax.random.uniform(jax.random.fold_in(own, dim), (shards_of,), jnp.float32, smallest / len(shards), high / len(shards)))
        gain = gain * jnp.repeat(steps, dims[dim] // shards_of).reshape([-1 if axis == dim else 1 for axis in range(len(dims))])
    return gain


def shared_out(rng, own, number, rows, amount, top, limit, lean):
    sequence = jax.random.permutation(rng, amount)
    packed, common = shares(amount, rows * top, limit, lean, True), shares(amount, rows * top, limit, lean, False)
    places = jnp.arange(amount)

    def named(sizes, turn):
        used = int((sizes > 0).sum())
        fixed = max(1, used // 4)
        passed = fixed + (places - fixed + turn * (used - fixed)) % max(1, amount - fixed)
        return jnp.zeros((amount,), jnp.int32).at[sequence[jnp.where(places < fixed, places, passed)]].set(jnp.asarray(sizes, jnp.int32))

    sizes = jnp.where(number % 4 == 0, named(packed, number // 4), named(common, number - number // 4 - 1))
    mixed = jax.random.permutation(jax.random.fold_in(own, 3), amount)
    donor, receiver = mixed[0:amount // 2 * 2:2], mixed[1:amount // 2 * 2:2]
    room = jnp.minimum(sizes[donor] - 1, limit - sizes[receiver]) // 2
    room = jnp.where((donor == sequence[0]) | (receiver == sequence[0]) | (sizes[receiver] == 0), 0, jnp.maximum(room, 0))
    passed = jax.random.randint(jax.random.fold_in(own, 4), (amount // 2,), 0, 1 << 20) % (room + 1)
    sizes = sizes.at[donor].add(-passed).at[receiver].add(passed)
    members = jnp.searchsorted(jnp.cumsum(sizes), jnp.arange(rows * top), side="right").astype(jnp.int32)
    listing = members.reshape(top, rows).T
    listing = listing[jax.random.permutation(jax.random.fold_in(own, 1), rows)]
    turn = jax.random.randint(jax.random.fold_in(own, 2), (rows, 1), 0, top)
    return jnp.take_along_axis(listing, (jnp.arange(top)[None, :] + turn) % top, axis=1)


def shares(count, total, most, slope, full):
    weights = [(1 << 20) // math.isqrt(standing ** slope) + 1 for standing in range(1, count + 1)]
    largest = most if full else min(most, max(-(-total // count), total * weights[0] // sum(weights)))
    least = 1 if total - largest >= count - 1 else 0
    holding, surplus = [largest] + [least] * (count - 1), total - largest - least * (count - 1)
    while surplus > 0:
        free = [i for i in range(1, count) if holding[i] < largest] or [i for i in range(1, count) if holding[i] < most]
        mass, left = sum([weights[i] for i in free]), surplus
        for i in free:
            more = min(most - holding[i], max(1, left * weights[i] // mass), surplus)
            holding[i] = holding[i] + more
            surplus = surplus - more
    return np.array(holding)


def centred(key, shape, deviation, reach, cuts=(), held_as=jnp.bfloat16):
    drawn = deviation * jax.random.normal(key, shape, jnp.float32)
    if cuts:
        drawn = drawn * block_scale(key, shape, cuts, -0.22, 0.18)
    return jnp.clip(drawn, -reach, reach).astype(held_as)


def setup_inputs(seed: int = 0) -> dict:
    streams_of = jax.random.split(jax.random.key(seed), 12)
    fwd_input = centred(streams_of[0], (SECTIONS, TOKENS, D), 1.0, 6.0, ((0, 4), (1, 4), (2, 32)))
    fresh_input = centred(streams_of[1], (TICKS - 1, TOKENS, D), 1.0, 6.0, ((1, 4), (2, 32)))
    fwd_experts_keys = jax.random.split(jax.random.fold_in(streams_of[2], 1), SECTIONS * TICKS * TOKENS // TOK_DEV)
    fwd_experts_turns = jax.random.permutation(jax.random.fold_in(streams_of[2], 3), SECTIONS * TICKS * TOKENS // TOK_DEV)
    fwd_experts = jax.vmap(lambda own, number: shared_out(jax.random.fold_in(streams_of[2], 2), own, number, TOK_DEV, EXPERTS, 2, CAP, 2))(fwd_experts_keys, fwd_experts_turns).reshape((SECTIONS, TICKS, TOKENS, 2))
    fwd_gates = jnp.clip(0.2 + 0.8 * jax.random.uniform(streams_of[3], (SECTIONS, TICKS, TOKENS, 2), jnp.float32) ** block_scale(streams_of[3], (SECTIONS, TICKS, TOKENS, 2), ((0, 4), (2, 4)), -0.2, 0.2), 0.2, 1.0)
    bwd_saved = centred(streams_of[4], (SECTIONS, TICKS, TOKENS, D), 1.0, 6.0, ((0, 4), (2, 4), (3, 32)))
    bwd_experts_keys = jax.random.split(jax.random.fold_in(streams_of[5], 1), SECTIONS * TICKS * TOKENS // TOK_DEV)
    bwd_experts_turns = jax.random.permutation(jax.random.fold_in(streams_of[5], 3), SECTIONS * TICKS * TOKENS // TOK_DEV)
    bwd_experts = jax.vmap(lambda own, number: shared_out(jax.random.fold_in(streams_of[5], 2), own, number, TOK_DEV, EXPERTS, 2, CAP, 2))(bwd_experts_keys, bwd_experts_turns).reshape((SECTIONS, TICKS, TOKENS, 2))
    bwd_gates = jnp.clip(0.2 + 0.8 * jax.random.uniform(streams_of[6], (SECTIONS, TICKS, TOKENS, 2), jnp.float32) ** block_scale(streams_of[6], (SECTIONS, TICKS, TOKENS, 2), ((0, 4), (2, 4)), -0.2, 0.2), 0.2, 1.0)
    out_grad = centred(streams_of[7], (SECTIONS, TOKENS, D), 1.0, 6.0, ((0, 4), (1, 4), (2, 32)))
    fresh_grad = centred(streams_of[8], (TICKS - 1, TOKENS, D), 1.0, 6.0, ((1, 4), (2, 32)))
    gate_proj = centred(streams_of[9], (SECTIONS, EXPERTS, FF, D), D ** -0.5, 0.125, ((0, 4), (1, 4), (2, 32)))
    down_proj = centred(streams_of[10], (SECTIONS, EXPERTS, FF, D), FF ** -0.5, 0.0625, ((0, 4), (1, 4), (2, 32)))
    return dict(fwd_input=fwd_input, fresh_input=fresh_input, fwd_experts=fwd_experts, fwd_gates=fwd_gates, bwd_saved=bwd_saved, bwd_experts=bwd_experts, bwd_gates=bwd_gates, out_grad=out_grad, fresh_grad=fresh_grad, gate_proj=gate_proj, down_proj=down_proj)


precise = lax.Precision.HIGHEST

def block_sum(hidden, weight, blocks):
    length = hidden.shape[0]
    pieces = jnp.einsum('tbf,bfd->tbd', hidden.astype(jnp.float32).reshape(length, blocks, -1), weight.astype(jnp.float32).reshape(blocks, -1, weight.shape[-1]), precision=precise)
    rounded = lax.optimization_barrier(pieces.astype(jnp.bfloat16))
    return lax.optimization_barrier(jnp.sum(rounded.astype(jnp.float32), axis=1))

def routed_weight(experts, gate_values, number):
    return lax.optimization_barrier(jnp.sum(jnp.where(experts == number, gate_values, jnp.float32(0.0)), axis=1))

def layer_forward(inputs, experts, gate_values, gate_weight, down_weight):
    combined = inputs.astype(jnp.float32)
    for number in range(EXPERTS):
        weight_row = routed_weight(experts, gate_values, number)
        before_act = jnp.dot(inputs, gate_weight[number].T, preferred_element_type=jnp.float32)
        hidden = jax.nn.silu(before_act).astype(jnp.bfloat16)
        output = block_sum(hidden, down_weight[number], BLOCKS)
        combined = combined + weight_row[:, None] * output
    return combined.astype(jnp.bfloat16)

def layer_backward(stored, experts, gate_values, cotangent, gate_weight, down_weight):
    result = cotangent.astype(jnp.float32)
    gate_parts = []
    down_parts = []
    for number in range(EXPERTS):
        weight_row = routed_weight(experts, gate_values, number)
        scaled = (weight_row[:, None] * cotangent.astype(jnp.float32)).astype(jnp.bfloat16)
        before_act = jnp.dot(stored, gate_weight[number].T, preferred_element_type=jnp.float32)
        hidden = jax.nn.silu(before_act).astype(jnp.bfloat16)
        down_parts.append(jnp.dot(hidden.T, scaled, preferred_element_type=jnp.float32))
        through = jnp.dot(scaled, down_weight[number].T, preferred_element_type=jnp.float32)
        sigmoid = jax.nn.sigmoid(before_act)
        slope_grad = (through * sigmoid * (1.0 + before_act * (1.0 - sigmoid))).astype(jnp.bfloat16)
        gate_parts.append(jnp.dot(slope_grad.T, stored, preferred_element_type=jnp.float32))
        result = result + block_sum(slope_grad, gate_weight[number], BLOCKS)
    return (result.astype(jnp.bfloat16), jnp.stack(gate_parts), jnp.stack(down_parts))

def reference(fwd_input, fresh_input, fwd_experts, fwd_gates, bwd_saved, bwd_experts, bwd_gates, out_grad, fresh_grad, gate_proj, down_proj):
    forward = [[None for tick_index in range(TICKS)] for section_index in range(SECTIONS)]
    backward = [[None for tick_index in range(TICKS)] for section_index in range(SECTIONS)]
    gate_sums = [jnp.zeros((EXPERTS, FF, D), jnp.float32) for section_index in range(SECTIONS)]
    down_sums = [jnp.zeros((EXPERTS, FF, D), jnp.float32) for section_index in range(SECTIONS)]
    for tick_index in range(TICKS):
        for section_index in range(SECTIONS):
            if tick_index == 0:
                inputs = fwd_input[section_index]
            elif section_index == 0:
                inputs = fresh_input[tick_index - 1]
            else:
                inputs = forward[section_index - 1][tick_index - 1]
            forward[section_index][tick_index] = layer_forward(inputs, fwd_experts[section_index, tick_index], fwd_gates[section_index, tick_index], gate_proj[section_index], down_proj[section_index])
            if tick_index == 0:
                cotangent = out_grad[section_index]
            elif section_index == SECTIONS - 1:
                cotangent = fresh_grad[tick_index - 1]
            else:
                cotangent = backward[section_index + 1][tick_index - 1]
            result, gate_step, down_step = layer_backward(bwd_saved[section_index, tick_index], bwd_experts[section_index, tick_index], bwd_gates[section_index, tick_index], cotangent, gate_proj[section_index], down_proj[section_index])
            backward[section_index][tick_index] = result
            gate_sums[section_index] = gate_sums[section_index] + gate_step
            down_sums[section_index] = down_sums[section_index] + down_step
    squares = jnp.float32(0.0)
    for section_index in range(SECTIONS):
        squares = squares + jnp.sum(gate_sums[section_index] * gate_sums[section_index]) + jnp.sum(down_sums[section_index] * down_sums[section_index])
    clip_limit = 0.25 * math.sqrt(2.0 * SECTIONS * EXPERTS * FF * D)
    factor = clip_limit / jnp.maximum(jnp.sqrt(squares), clip_limit)
    fwd_output = jnp.stack([jnp.stack(forward[section_index]) for section_index in range(SECTIONS)])
    input_grad = jnp.stack([jnp.stack(backward[section_index]) for section_index in range(SECTIONS)])
    gate_grad = (jnp.stack(gate_sums) * factor).astype(jnp.bfloat16)
    down_grad = (jnp.stack(down_sums) * factor).astype(jnp.bfloat16)
    return (fwd_output, input_grad, gate_grad, down_grad)
```

```python
import math

import jax
import jax.numpy as jnp
from jax import lax
from jax.experimental import pallas as pl
from jax.experimental.pallas import tpu as pltpu
from jax.sharding import Mesh
from jax.sharding import PartitionSpec as P

D = 2048
FF = 7168
EXPERTS = 4
EXPERT = ("z", "core")
BF = jnp.bfloat16
F32 = jnp.float32
CHUNKS = 16
LANES = 128
ROWS = 32
TOKS = EXPERTS * ROWS
HID = 224

NT = (((1,), (1,)), ((), ()))
TN = (((0,), (0,)), ((), ()))


def call(body, outs, *args, scratch=(), limit=32):
    vmem = pl.BlockSpec(memory_space=pltpu.VMEM)
    return pl.pallas_call(
        body,
        out_shape=outs,
        in_specs=[vmem] * len(args),
        out_specs=jax.tree.map(lambda _: vmem, outs),
        scratch_shapes=list(scratch),
        compiler_params=pltpu.CompilerParams(vmem_limit_bytes=limit * 1024 * 1024),
    )(*args)


def shaped(shape, dtype):
    return jax.ShapeDtypeStruct(shape, dtype)


def spread_body(got, weight, out):
    rows = got.shape[1]
    for e in range(EXPERTS):
        scale = weight[e]
        for k in range(CHUNKS):
            out[e, k, 0:ROWS, :] = got[k, 0:ROWS, :]
            out[e, k, ROWS : 2 * ROWS, :] = (scale * got[k, ROWS : 2 * ROWS, :].astype(F32)).astype(BF)
            if rows > 2 * ROWS:
                out[e, k, 2 * ROWS : rows, :] = got[k, 2 * ROWS : rows, :]


def spread(got, weight):
    return call(spread_body, shaped((EXPERTS, *got.shape), BF), got, weight)


def layer_body(stored_at, came, kept, gate_own, gate_other, down_own, down_other, out, own, other, both, grad):
    for e in range(EXPERTS):
        for k in range(CHUNKS):
            lanes = slice(k * LANES, (k + 1) * LANES)
            both[e * ROWS : (e + 1) * ROWS, lanes] = came[e, k, 0:ROWS, :]
            both[TOKS + e * ROWS : TOKS + (e + 1) * ROWS, lanes] = kept[e, k, stored_at : stored_at + ROWS, :]
            grad[e * ROWS : (e + 1) * ROWS, lanes] = came[e, k, ROWS : 2 * ROWS, :]
    tokens, cotangent = both[...], grad[...]
    hidden_fwd, slopes = [], []
    for gate, down, keep in ((gate_own, down_own, own), (gate_other, down_other, other)):
        before = lax.dot_general(tokens, gate[...], NT, preferred_element_type=F32)
        sigmoid = 1.0 / (1.0 + jnp.exp(-before))
        hidden = (before * sigmoid).astype(BF)
        hidden_fwd.append(hidden[0:TOKS])
        through = lax.dot_general(cotangent, down[...], NT, preferred_element_type=F32)
        sig, pre = sigmoid[TOKS:], before[TOKS:]
        slope = (through * sig * (1.0 + pre * (1.0 - sig))).astype(BF)
        slopes.append(slope)
        keep[0] = hidden[TOKS:]
        keep[1] = slope
    forward = jnp.dot(hidden_fwd[0], down_own[...], preferred_element_type=F32) + jnp.dot(
        hidden_fwd[1], down_other[...], preferred_element_type=F32
    )
    backward = jnp.dot(slopes[0], gate_own[...], preferred_element_type=F32) + jnp.dot(
        slopes[1], gate_other[...], preferred_element_type=F32
    )
    forward, backward = forward.astype(BF), backward.astype(BF)
    for e in range(EXPERTS):
        for k in range(CHUNKS):
            rows, lanes = slice(e * ROWS, (e + 1) * ROWS), slice(k * LANES, (k + 1) * LANES)
            out[e, k, 0:ROWS, :] = forward[rows, lanes]
            out[e, k, ROWS : 2 * ROWS, :] = backward[rows, lanes]


def layer(came, kept, stored_at, weights):
    def body(*refs):
        layer_body(stored_at, *refs)

    pair = shaped((2, TOKS, HID), BF)
    return call(
        body,
        (shaped((EXPERTS, CHUNKS, 2 * ROWS, LANES), BF), pair, pair),
        came,
        kept,
        *weights,
        scratch=(pltpu.VMEM((2 * TOKS, D), BF), pltpu.VMEM((TOKS, D), BF)),
    )


def combine_chunks(back, weight, out):
    for k in range(CHUNKS):
        fwd = weight[0] * back[0, k, 0:ROWS, :].astype(F32)
        bwd = back[0, k, ROWS : 2 * ROWS, :].astype(F32)
        for e in range(1, EXPERTS):
            fwd = fwd + weight[e] * back[e, k, 0:ROWS, :].astype(F32)
            bwd = bwd + back[e, k, ROWS : 2 * ROWS, :].astype(F32)
        out[k, 0:ROWS, :] = fwd.astype(BF)
        out[k, ROWS : 2 * ROWS, :] = bwd.astype(BF)


def combine_sum_body(back, weight, squares, out):
    combine_chunks(back, weight, out)
    total = jnp.full((16, LANES), jnp.sum(squares[...]), F32)
    high = total.astype(BF).astype(F32)
    middle = (total - high).astype(BF).astype(F32)
    low = total - high - middle
    row = lax.broadcasted_iota(jnp.int32, (16, LANES), 0)
    zero = jnp.zeros((16, LANES), F32)
    pieces = jnp.where(row == 0, high, jnp.where(row == 1, middle, jnp.where(row == 2, low, zero))).astype(BF)
    for k in range(CHUNKS):
        out[k, 2 * ROWS : 2 * ROWS + 16, :] = pieces


def combine(back, weight, squares=None):
    if squares is None:
        return call(combine_chunks, shaped((CHUNKS, 2 * ROWS, LANES), BF), back, weight)
    return call(combine_sum_body, shaped((CHUNKS, 2 * ROWS + 16, LANES), BF), back, weight, squares)


def grads_body(came0, came0p, came1, came1p, own0, own0p, own1, own1p, gate, down, squares, cot, stored):
    sources = ((came0, came0, 2), (came0p, came0p, 2), (came1, came0, 3), (came1p, came0p, 3))
    for n, (came, kept, at) in enumerate(sources):
        for e in range(EXPERTS):
            for k in range(CHUNKS):
                rows = slice(n * TOKS + e * ROWS, n * TOKS + (e + 1) * ROWS)
                lanes = slice(k * LANES, (k + 1) * LANES)
                cot[rows, lanes] = came[e, k, ROWS : 2 * ROWS, :]
                stored[rows, lanes] = kept[e, k, at * ROWS : (at + 1) * ROWS, :]
    pairs = (own0, own0p, own1, own1p)
    hidden = jnp.concatenate([p[0] for p in pairs], axis=0)
    slope = jnp.concatenate([p[1] for p in pairs], axis=0)
    total = jnp.zeros((8, LANES), F32)
    width = 512
    for at in range(0, D, width):
        lanes = slice(at, at + width)
        for left, right, out in ((slope, stored, gate), (hidden, cot, down)):
            part = lax.dot_general(left, right[:, lanes], TN, preferred_element_type=F32)
            out[:, lanes] = part
            square = jnp.sum((part * part).reshape(HID // 8, 8, width), axis=0)
            for lane in range(0, width, LANES):
                total = total + square[:, lane : lane + LANES]
    squares[...] = total


def grads(*args):
    out = shaped((HID, D), F32)
    tokens = 4 * TOKS
    return call(
        grads_body,
        (out, out, shaped((8, LANES), F32)),
        *args,
        scratch=(pltpu.VMEM((tokens, D), BF), pltpu.VMEM((tokens, D), BF)),
        limit=40,
    )


def swapped(value):
    return lax.ppermute(value, "core", [(0, 1), (1, 0)])


def shifted(value, steps):
    count = lax.axis_size("section")
    return lax.ppermute(
        value, "section", [(s, s + steps) for s in range(max(0, -steps), min(count, count - steps))]
    )


def to_everyone(value, axis):
    return lax.all_to_all(
        jnp.broadcast_to(value[None], (lax.axis_size(axis), *value.shape)), axis, 0, 0, tiled=True
    )


def gate_rows(experts, gate_values):
    half = lax.axis_index("core") * ROWS
    experts = lax.dynamic_slice_in_dim(experts, half, ROWS, 1)
    gate_values = lax.dynamic_slice_in_dim(gate_values, half, ROWS, 1)
    number = jnp.arange(EXPERTS, dtype=jnp.int32)[None, :, None, None]
    rows = jnp.sum(jnp.where(experts[:, None] == number, gate_values[:, None], F32(0.0)), axis=-1)
    return jnp.broadcast_to(rows[..., None], (*rows.shape, LANES))


def on_device(
    fwd_input,
    fresh_input,
    fwd_experts,
    fwd_gates,
    bwd_saved,
    bwd_experts,
    bwd_gates,
    out_grad,
    fresh_grad,
    gate_proj,
    down_proj,
):
    gate_own, down_own = gate_proj[0, 0], down_proj[0, 0]
    section_count = lax.axis_size("section")
    section_index = lax.axis_index("section")
    is_first = section_index == 0
    is_last = section_index == section_count - 1

    streams = jnp.concatenate([fwd_input, out_grad, bwd_saved[0], fresh_input, fresh_grad], axis=0)
    count = streams.shape[0]
    halves = jnp.moveaxis(streams.reshape(count, 2, ROWS, 64), 1, 0)
    met = lax.all_to_all(halves, "core", 0, 0, tiled=True)
    packed = jnp.concatenate([met[0], met[1]], axis=-1)
    first = packed[0:4].reshape(4 * ROWS, LANES)
    fresh = packed[4:6].reshape(2 * ROWS, LANES)

    gate_other, down_other = swapped(gate_own), swapped(down_own)
    weights = (gate_own, gate_other, down_own, down_other)
    fwd_weight = gate_rows(fwd_experts[0], fwd_gates[0])
    bwd_weight = gate_rows(bwd_experts[0], bwd_gates[0])

    got = to_everyone(first, "z")
    came0 = lax.all_to_all(spread(got, bwd_weight[0]), "dp", 0, 0, tiled=True)
    came0p = swapped(came0)
    partial, own0, other0 = layer(came0, came0, 2 * ROWS, weights)
    own0p = swapped(other0)
    back = lax.all_to_all(partial, "dp", 0, 0, tiled=True)
    pieces = lax.all_to_all(combine(back, fwd_weight[0]), "z", 0, 0, tiled=True)
    base = first[0 : 2 * ROWS]
    result0 = (base.astype(F32) + jnp.sum(pieces.astype(F32), axis=0)).astype(BF)

    arriving = shifted(result0[0:ROWS], 1)
    leaving = shifted(result0[ROWS : 2 * ROWS], -1)
    second = jnp.concatenate(
        [
            jnp.where(is_first, fresh[0:ROWS], arriving),
            jnp.where(is_last, fresh[ROWS : 2 * ROWS], leaving),
        ],
        axis=0,
    )

    got = to_everyone(second, "z")
    came1 = lax.all_to_all(spread(got, bwd_weight[1]), "dp", 0, 0, tiled=True)
    came1p = swapped(came1)
    partial, own1, other1 = layer(came1, came0, 3 * ROWS, weights)
    own1p = swapped(other1)
    back = lax.all_to_all(partial, "dp", 0, 0, tiled=True)
    gate_total, down_total, squares = grads(
        came0, came0p, came1, came1p, own0, own0p, own1, own1p
    )
    pieces = lax.all_to_all(combine(back, fwd_weight[1], squares), "z", 0, 0, tiled=True)
    sent = pieces[:, 0 : 2 * ROWS].astype(F32)
    result1 = (second.astype(F32) + jnp.sum(sent, axis=0)).astype(BF)

    along_z = jnp.sum(pieces[:, 2 * ROWS : 2 * ROWS + 3, 0].astype(F32))
    plane = ("section", "dp", "core")
    tiles = lax.all_to_all(
        jnp.full((32, 8, LANES), along_z, F32), plane, 0, 0, tiled=True
    )
    total = jnp.sum(tiles[:, 0, 0])
    clip_limit = 0.25 * math.sqrt(2.0 * section_count * EXPERTS * FF * D)
    factor = clip_limit / jnp.maximum(jnp.sqrt(total), clip_limit)
    gate_grad = (gate_total * factor).astype(BF)[None, None]
    down_grad = (down_total * factor).astype(BF)[None, None]

    results = jnp.stack([result0, result1]).reshape(2, 2, ROWS, 2, 64)
    homed = lax.all_to_all(jnp.moveaxis(results, 3, 0), "core", 0, 0, tiled=True)
    final = jnp.transpose(homed, (2, 1, 0, 3, 4)).reshape(2, 1, 2, 2 * ROWS, 64)
    return (final[0], final[1], gate_grad, down_grad)


def solution(mesh):
    split = Mesh(
        mesh.devices.reshape(mesh.shape["section"], CHUNKS, 2, mesh.shape["dp"]),
        ("section", "z", "core", "dp"),
    )
    return jax.shard_map(
        on_device,
        mesh=split,
        in_specs=(
            P("section", "dp", EXPERT),
            P(None, "dp", EXPERT),
            P("section", None, "dp", None),
            P("section", None, "dp", None),
            P("section", None, "dp", EXPERT),
            P("section", None, "dp", None),
            P("section", None, "dp", None),
            P("section", "dp", EXPERT),
            P(None, "dp", EXPERT),
            P("section", "dp", EXPERT, None),
            P("section", "dp", EXPERT, None),
        ),
        out_specs=(
            P("section", None, "dp", EXPERT),
            P("section", None, "dp", EXPERT),
            P("section", "dp", EXPERT, None),
            P("section", "dp", EXPERT, None),
        ),
        check_vma=False,
    )
```

```python
import math

import jax
import jax.numpy as jnp
from jax import lax
from jax.experimental import pallas as pl
from jax.experimental.pallas import tpu as pltpu
from jax.sharding import Mesh
from jax.sharding import PartitionSpec as P

D = 2048
FF = 7168
EXPERTS = 4
EXPERT = ("z", "core")
BF = jnp.bfloat16
F32 = jnp.float32
CHUNKS = 16
LANES = 128
ROWS = 32
TOKS = EXPERTS * ROWS
HID = 224

NT = (((1,), (1,)), ((), ()))
TN = (((0,), (0,)), ((), ()))


VMEM, HBM, SMEM = pltpu.VMEM, pltpu.HBM, pltpu.SMEM


def call(body, outs, args, scratch=(), limit=24):
    return pl.pallas_call(
        body,
        out_shape=tuple(jax.ShapeDtypeStruct(shape, dtype) for shape, dtype, _ in outs),
        in_specs=[pl.BlockSpec(memory_space=space) for _, space in args],
        out_specs=tuple(pl.BlockSpec(memory_space=space) for _, _, space in outs),
        scratch_shapes=list(scratch),
        compiler_params=pltpu.CompilerParams(vmem_limit_bytes=limit * 1024 * 1024),
    )(*(array for array, _ in args))


def sems(number):
    return pltpu.SemaphoreType.DMA((number,))


def halves(first, own, other):
    return jnp.where(first, jnp.concatenate([own, other], -1), jnp.concatenate([other, own], -1))


def pack_body(core, *refs):
    inputs, (send, keep) = refs[:-2], refs[-2:]
    mine = pl.multiple_of(core[0] * ROWS, ROWS)
    others = pl.multiple_of((1 - core[0]) * ROWS, ROWS)
    at = 0
    for ref in inputs:
        for n in range(ref.shape[0]):
            keep[at] = ref[n, pl.ds(mine, ROWS), :]
            send[at] = ref[n, pl.ds(others, ROWS), :]
            at += 1


def pack(core, arrays):
    count = sum(a.shape[0] for a in arrays)
    shape = (count, ROWS, 64)
    return call(
        pack_body,
        ((shape, BF, VMEM), (shape, BF, VMEM)),
        ((core, SMEM), *((a, VMEM) for a in arrays)),
    )


def open_body(core, keep, got, out, first, fresh, arrived):
    lead = jnp.full((ROWS, LANES), core[0], jnp.int32) == 0
    for n in range(6):
        rows = halves(lead, keep[n].astype(F32), got[n].astype(F32)).astype(BF)
        if n < 4:
            first[n * ROWS : (n + 1) * ROWS, :] = rows
        else:
            fresh[(n - 4) * ROWS : (n - 3) * ROWS, :] = rows
    copies = [pltpu.make_async_copy(first, out.at[k], arrived.at[k]) for k in range(CHUNKS)]
    for c in copies:
        c.start()
    for c in copies:
        c.wait()


def opened(core, keep, got):
    return call(
        open_body,
        (
            ((CHUNKS, 4 * ROWS, LANES), BF, HBM),
            ((4 * ROWS, LANES), BF, VMEM),
            ((2 * ROWS, LANES), BF, VMEM),
        ),
        ((core, SMEM), (keep, VMEM), (got, VMEM)),
        scratch=(sems(CHUNKS),),
    )


def next_body(place, arriving, leaving, fresh, out, second, arrived):
    at_first = jnp.full((ROWS, LANES), place[0], jnp.int32) == 0
    at_last = jnp.full((ROWS, LANES), place[1], jnp.int32) == 0
    second[0:ROWS, :] = jnp.where(at_first, fresh[0:ROWS, :].astype(F32), arriving[...].astype(F32)).astype(BF)
    second[ROWS : 2 * ROWS, :] = jnp.where(
        at_last, fresh[ROWS : 2 * ROWS, :].astype(F32), leaving[...].astype(F32)
    ).astype(BF)
    copies = [pltpu.make_async_copy(second, out.at[k], arrived.at[k]) for k in range(CHUNKS)]
    for c in copies:
        c.start()
    for c in copies:
        c.wait()


def following(place, arriving, leaving, fresh):
    return call(
        next_body,
        (((CHUNKS, 2 * ROWS, LANES), BF, HBM), ((2 * ROWS, LANES), BF, VMEM)),
        ((place, SMEM), (arriving, VMEM), (leaving, VMEM), (fresh, VMEM)),
        scratch=(sems(CHUNKS),),
    )


def spread_body(got, weight, out, staged, sent):
    rows = got.shape[1]
    copies = []
    for e in range(EXPERTS):
        scale = weight[e]
        for k in range(CHUNKS):
            staged[e, k, 0:ROWS, :] = got[k, 0:ROWS, :]
            staged[e, k, ROWS : 2 * ROWS, :] = (scale * got[k, ROWS : 2 * ROWS, :].astype(F32)).astype(BF)
            if rows > 2 * ROWS:
                staged[e, k, 2 * ROWS : rows, :] = got[k, 2 * ROWS : rows, :]
        copies.append(pltpu.make_async_copy(staged.at[e], out.at[e], sent.at[e]))
        copies[-1].start()
    for c in copies:
        c.wait()


def spread(got, weight):
    shape = (EXPERTS, *got.shape)
    return call(
        spread_body,
        ((shape, BF, HBM),),
        ((got, VMEM), (weight, VMEM)),
        scratch=(pltpu.VMEM(shape, BF), sems(EXPERTS)),
    )[0]


def layer_body(kept_at, came, *refs):
    refs = list(refs)
    kept = refs.pop(0) if kept_at is not None else None
    gate_own, gate_other, down_own, down_other, out, own, other = refs[:7]
    both, grad, staged, g_own, g_other, d_own, d_other, sent, loaded = refs[7:16]
    loads = [
        pltpu.make_async_copy(s, d, loaded.at[n])
        for n, (s, d) in enumerate(
            ((gate_own, g_own), (down_own, d_own), (gate_other, g_other), (down_other, d_other))
        )
    ]
    if kept_at is not None:
        stored = refs[16]
        loads.append(
            pltpu.make_async_copy(kept.at[:, :, pl.ds(kept_at, ROWS), :], stored, loaded.at[4])
        )
        loads[4].start()
    for c in loads[0:4]:
        c.start()
    for e in range(EXPERTS):
        for k in range(CHUNKS):
            lanes = slice(k * LANES, (k + 1) * LANES)
            both[e * ROWS : (e + 1) * ROWS, lanes] = came[e, k, 0:ROWS, :]
            grad[e * ROWS : (e + 1) * ROWS, lanes] = came[e, k, ROWS : 2 * ROWS, :]
            if kept_at is None:
                both[TOKS + e * ROWS : TOKS + (e + 1) * ROWS, lanes] = came[e, k, 2 * ROWS : 3 * ROWS, :]
    if kept_at is not None:
        loads[4].wait()
        for e in range(EXPERTS):
            for k in range(CHUNKS):
                lanes = slice(k * LANES, (k + 1) * LANES)
                both[TOKS + e * ROWS : TOKS + (e + 1) * ROWS, lanes] = stored[e, k]
    tokens, cotangent = both[...], grad[...]
    hidden_fwd, slopes = [], []
    for n, (gate, down, keep) in enumerate(((g_own, d_own, own), (g_other, d_other, other))):
        loads[2 * n].wait()
        before = lax.dot_general(tokens, gate[...], NT, preferred_element_type=F32)
        sigmoid = 1.0 / (1.0 + jnp.exp(-before))
        hidden = (before * sigmoid).astype(BF)
        hidden_fwd.append(hidden[0:TOKS])
        loads[2 * n + 1].wait()
        through = lax.dot_general(cotangent, down[...], NT, preferred_element_type=F32)
        sig, pre = sigmoid[TOKS:], before[TOKS:]
        slope = (through * sig * (1.0 + pre * (1.0 - sig))).astype(BF)
        slopes.append(slope)
        keep[0] = hidden[TOKS:]
        keep[1] = slope
    forward = jnp.dot(hidden_fwd[0], d_own[...], preferred_element_type=F32) + jnp.dot(
        hidden_fwd[1], d_other[...], preferred_element_type=F32
    )
    backward = jnp.dot(slopes[0], g_own[...], preferred_element_type=F32) + jnp.dot(
        slopes[1], g_other[...], preferred_element_type=F32
    )
    forward, backward = forward.astype(BF), backward.astype(BF)
    stores = []
    for e in range(EXPERTS):
        for k in range(CHUNKS):
            rows, lanes = slice(e * ROWS, (e + 1) * ROWS), slice(k * LANES, (k + 1) * LANES)
            staged[e, k, 0:ROWS, :] = forward[rows, lanes]
            staged[e, k, ROWS : 2 * ROWS, :] = backward[rows, lanes]
        stores.append(pltpu.make_async_copy(staged.at[e], out.at[e], sent.at[e]))
        stores[-1].start()
    for c in stores:
        c.wait()


def layer(came, kept, kept_at, weights):
    def body(*refs):
        layer_body(kept_at, *refs)

    shape = (EXPERTS, CHUNKS, 2 * ROWS, LANES)
    pair = (2, TOKS, HID)
    weight = pltpu.VMEM((HID, D), BF)
    scratch = [
        pltpu.VMEM((2 * TOKS, D), BF),
        pltpu.VMEM((TOKS, D), BF),
        pltpu.VMEM(shape, BF),
        *([weight] * 4),
        sems(EXPERTS),
        sems(5),
    ]
    args = [(came, VMEM)]
    if kept_at is not None:
        scratch.append(pltpu.VMEM((EXPERTS, CHUNKS, ROWS, LANES), BF))
        args.append((kept, HBM))
    return call(
        body,
        ((shape, BF, HBM), (pair, BF, VMEM), (pair, BF, VMEM)),
        (*args, *((w, HBM) for w in weights)),
        scratch=scratch,
    )


def combine_chunks(back, weight, out):
    for k in range(CHUNKS):
        fwd = weight[0] * back[0, k, 0:ROWS, :].astype(F32)
        bwd = back[0, k, ROWS : 2 * ROWS, :].astype(F32)
        for e in range(1, EXPERTS):
            fwd = fwd + weight[e] * back[e, k, 0:ROWS, :].astype(F32)
            bwd = bwd + back[e, k, ROWS : 2 * ROWS, :].astype(F32)
        out[k, 0:ROWS, :] = fwd.astype(BF)
        out[k, ROWS : 2 * ROWS, :] = bwd.astype(BF)


def combine_body(back, weight, out, staged, sent):
    combine_chunks(back, weight, staged)
    c = pltpu.make_async_copy(staged, out, sent.at[0])
    c.start()
    c.wait()


def combine_sum_body(back, weight, squares, out, staged, sent):
    combine_chunks(back, weight, staged)
    total = jnp.full((16, LANES), jnp.sum(squares[...]), F32)
    high = total.astype(BF).astype(F32)
    middle = (total - high).astype(BF).astype(F32)
    low = total - high - middle
    row = lax.broadcasted_iota(jnp.int32, (16, LANES), 0)
    zero = jnp.zeros((16, LANES), F32)
    pieces = jnp.where(row == 0, high, jnp.where(row == 1, middle, jnp.where(row == 2, low, zero))).astype(BF)
    for k in range(CHUNKS):
        staged[k, 2 * ROWS : 2 * ROWS + 16, :] = pieces
    c = pltpu.make_async_copy(staged, out, sent.at[0])
    c.start()
    c.wait()


def combine(back, weight, squares=None):
    shape = (CHUNKS, 2 * ROWS + (16 if squares is not None else 0), LANES)
    args = [(back, VMEM), (weight, VMEM)]
    if squares is not None:
        args.append((squares, VMEM))
    return call(
        combine_body if squares is None else combine_sum_body,
        ((shape, BF, HBM),),
        args,
        scratch=(pltpu.VMEM(shape, BF), sems(1)),
    )[0]


def grads_body(
    came0, came0p, came1, came1p, own0, own0p, own1, own1p, gate, down, squares,
    buf0, buf0p, buf1, buf1p, cot, stored, gate_v, down_v, loaded, sent,
):
    tail = pl.ds(ROWS, 3 * ROWS)
    one = pl.ds(ROWS, ROWS)
    loads = [
        pltpu.make_async_copy(came0.at[:, :, tail, :], buf0, loaded.at[0]),
        pltpu.make_async_copy(came0p.at[:, :, tail, :], buf0p, loaded.at[1]),
        pltpu.make_async_copy(came1.at[:, :, one, :], buf1, loaded.at[2]),
        pltpu.make_async_copy(came1p.at[:, :, one, :], buf1p, loaded.at[3]),
    ]
    for c in loads:
        c.start()
    sources = ((buf0, buf0, 1), (buf0p, buf0p, 1), (buf1, buf0, 2), (buf1p, buf0p, 2))
    for n, (came, kept, at) in enumerate(sources):
        loads[n].wait()
        for e in range(EXPERTS):
            for k in range(CHUNKS):
                rows = slice(n * TOKS + e * ROWS, n * TOKS + (e + 1) * ROWS)
                lanes = slice(k * LANES, (k + 1) * LANES)
                cot[rows, lanes] = came[e, k, 0:ROWS, :]
                stored[rows, lanes] = kept[e, k, at * ROWS : (at + 1) * ROWS, :]
    pairs = (own0, own0p, own1, own1p)
    hidden = jnp.concatenate([p[0] for p in pairs], axis=0)
    slope = jnp.concatenate([p[1] for p in pairs], axis=0)
    total = jnp.zeros((8, LANES), F32)
    width = 512
    stores = []
    for n, at in enumerate(range(0, D, width)):
        lanes = slice(at, at + width)
        for m, (left, right, out, held) in enumerate(
            ((slope, stored, gate, gate_v), (hidden, cot, down, down_v))
        ):
            part = lax.dot_general(left, right[:, lanes], TN, preferred_element_type=F32)
            held[:, lanes] = part
            stores.append(
                pltpu.make_async_copy(
                    held.at[:, pl.ds(at, width)], out.at[:, pl.ds(at, width)], sent.at[2 * n + m]
                )
            )
            stores[-1].start()
            square = jnp.sum((part * part).reshape(HID // 8, 8, width), axis=0)
            for lane in range(0, width, LANES):
                total = total + square[:, lane : lane + LANES]
    squares[...] = total
    for c in stores:
        c.wait()


def grads(cames, owns):
    tokens = 4 * TOKS
    total = ((HID, D), F32, HBM)
    return call(
        grads_body,
        (total, total, ((8, LANES), F32, VMEM)),
        (*((c, HBM) for c in cames), *((o, VMEM) for o in owns)),
        scratch=(
            pltpu.VMEM((EXPERTS, CHUNKS, 3 * ROWS, LANES), BF),
            pltpu.VMEM((EXPERTS, CHUNKS, 3 * ROWS, LANES), BF),
            pltpu.VMEM((EXPERTS, CHUNKS, ROWS, LANES), BF),
            pltpu.VMEM((EXPERTS, CHUNKS, ROWS, LANES), BF),
            pltpu.VMEM((tokens, D), BF),
            pltpu.VMEM((tokens, D), BF),
            pltpu.VMEM((HID, D), F32),
            pltpu.VMEM((HID, D), F32),
            sems(4),
            sems(8),
        ),
    )


def close_body(pieces, base, result, tiles):
    total = base[...].astype(F32)
    extra = jnp.zeros((16, LANES), F32)
    for k in range(CHUNKS):
        total = total + pieces[k, 0 : 2 * ROWS, :].astype(F32)
        extra = extra + pieces[k, 2 * ROWS : 2 * ROWS + 16, :].astype(F32)
    result[...] = total.astype(BF)
    along = jnp.sum(extra, axis=0, keepdims=True)
    for k in range(tiles.shape[0]):
        tiles[k] = jnp.broadcast_to(along, (8, LANES))


def closed(pieces, base, count):
    return call(
        close_body,
        (((2 * ROWS, LANES), BF, VMEM), ((count, 8, LANES), F32, VMEM)),
        ((pieces, VMEM), (base, VMEM)),
    )


STEP = 32


def clip_body(limit, tiles, gate, down, gate_out, down_out, gate_v, down_v, gate_o, down_o, loaded, sent):
    work = [
        (held, kept, out, pl.ds(at, STEP), pltpu.make_async_copy(
            source.at[pl.ds(at, STEP)], held.at[pl.ds(at, STEP)], loaded.at[m * (HID // STEP) + n]
        ))
        for n, at in enumerate(range(0, HID, STEP))
        for m, (source, held, kept, out) in enumerate(
            ((gate, gate_v, gate_o, gate_out), (down, down_v, down_o, down_out))
        )
    ]
    for *_, c in work:
        c.start()
    total = jnp.sum(tiles[...], axis=0)
    factor = (limit / jnp.maximum(jnp.sqrt(total), limit))[0:1, 0:1]
    stores = []
    for n, (held, kept, out, rows, c) in enumerate(work):
        c.wait()
        kept[rows, :] = (held[rows, :] * factor).astype(BF)
        stores.append(pltpu.make_async_copy(kept.at[rows], out.at[rows], sent.at[n]))
        stores[-1].start()
    for c in stores:
        c.wait()


def clipped(limit, tiles, gate, down):
    def body(*refs):
        clip_body(limit, *refs)

    number = 2 * (HID // STEP)
    out = ((HID, D), BF, HBM)
    return call(
        body,
        (out, out),
        ((tiles, VMEM), (gate, HBM), (down, HBM)),
        scratch=(
            pltpu.VMEM((HID, D), F32),
            pltpu.VMEM((HID, D), F32),
            pltpu.VMEM((HID, D), BF),
            pltpu.VMEM((HID, D), BF),
            sems(number),
            sems(number),
        ),
    )


def swapped(value):
    return lax.ppermute(value, "core", [(0, 1), (1, 0)])


def shifted(value, steps):
    count = lax.axis_size("section")
    return lax.ppermute(
        value, "section", [(s, s + steps) for s in range(max(0, -steps), min(count, count - steps))]
    )


def lanes_home(result, first):
    rows = result.reshape(2, ROWS, 2, 64)
    low, high = rows[:, :, 0], rows[:, :, 1]
    got = swapped(jnp.where(first, high, low))
    mine = jnp.where(first, low, high)
    return jnp.where(first, jnp.concatenate([mine, got], 1), jnp.concatenate([got, mine], 1))


def gate_rows(experts, gate_values):
    half = lax.axis_index("core") * ROWS
    experts = lax.dynamic_slice_in_dim(experts, half, ROWS, 1)
    gate_values = lax.dynamic_slice_in_dim(gate_values, half, ROWS, 1)
    number = jnp.arange(EXPERTS, dtype=jnp.int32)[None, :, None, None]
    rows = jnp.sum(jnp.where(experts[:, None] == number, gate_values[:, None], F32(0.0)), axis=-1)
    return jnp.broadcast_to(rows[..., None], (*rows.shape, LANES))


def on_device(
    fwd_input,
    fresh_input,
    fwd_experts,
    fwd_gates,
    bwd_saved,
    bwd_experts,
    bwd_gates,
    out_grad,
    fresh_grad,
    gate_proj,
    down_proj,
):
    gate_own, down_own = gate_proj[0, 0], down_proj[0, 0]
    section_count = lax.axis_size("section")
    section_index = lax.axis_index("section")

    core_index = lax.axis_index("core").astype(jnp.int32)
    core = core_index[None]
    place = jnp.stack([section_index, section_count - 1 - section_index]).astype(jnp.int32)

    send, keep = pack(core, (fwd_input, out_grad, bwd_saved[0], fresh_input, fresh_grad))
    outgoing, first, fresh = opened(core, keep, swapped(send))

    weights = (gate_own, swapped(gate_own), down_own, swapped(down_own))
    fwd_weight = gate_rows(fwd_experts[0], fwd_gates[0])
    bwd_weight = gate_rows(bwd_experts[0], bwd_gates[0])

    got = lax.all_to_all(outgoing, "z", 0, 0, tiled=True)
    came0 = lax.all_to_all(spread(got, bwd_weight[0]), "dp", 0, 0, tiled=True)
    partial, own0, other0 = layer(came0, None, None, weights)
    came0, partial = lax.optimization_barrier((came0, partial))
    came0p, own0p = swapped(came0), swapped(other0)
    back = lax.all_to_all(partial, "dp", 0, 0, tiled=True)
    pieces = lax.all_to_all(combine(back, fwd_weight[0]), "z", 0, 0, tiled=True)
    base = first[0 : 2 * ROWS]
    result0 = (base.astype(F32) + jnp.sum(pieces.astype(F32), axis=0)).astype(BF)

    arriving = shifted(result0[0:ROWS], 1)
    leaving = shifted(result0[ROWS : 2 * ROWS], -1)
    outgoing, second = following(place, arriving, leaving, fresh)

    got = lax.all_to_all(outgoing, "z", 0, 0, tiled=True)
    came1 = lax.all_to_all(spread(got, bwd_weight[1]), "dp", 0, 0, tiled=True)
    partial, own1, other1 = layer(came1, came0, 3 * ROWS, weights)
    came1, partial = lax.optimization_barrier((came1, partial))
    came1p, own1p = swapped(came1), swapped(other1)
    back = lax.all_to_all(partial, "dp", 0, 0, tiled=True)
    gate_total, down_total, squares = grads(
        (came0, came0p, came1, came1p), (own0, own0p, own1, own1p)
    )
    pieces = lax.all_to_all(combine(back, fwd_weight[1], squares), "z", 0, 0, tiled=True)

    plane = ("section", "dp", "core")
    result1, tiles = closed(pieces, second, 32)
    tiles = lax.all_to_all(tiles, plane, 0, 0, tiled=True)
    clip_limit = 0.25 * math.sqrt(2.0 * section_count * EXPERTS * FF * D)
    gate_grad, down_grad = clipped(clip_limit, tiles, gate_total, down_total)

    leads = core_index == 0
    home0, home1 = lanes_home(result0, leads), lanes_home(result1, leads)
    fwd_output = jnp.stack([home0[0], home1[0]])[None]
    input_grad = jnp.stack([home0[1], home1[1]])[None]
    return (fwd_output, input_grad, gate_grad[None, None], down_grad[None, None])


def solution(mesh):
    split = Mesh(
        mesh.devices.reshape(mesh.shape["section"], CHUNKS, 2, mesh.shape["dp"]),
        ("section", "z", "core", "dp"),
    )
    return jax.shard_map(
        on_device,
        mesh=split,
        in_specs=(
            P("section", "dp", EXPERT),
            P(None, "dp", EXPERT),
            P("section", None, "dp", None),
            P("section", None, "dp", None),
            P("section", None, "dp", EXPERT),
            P("section", None, "dp", None),
            P("section", None, "dp", None),
            P("section", "dp", EXPERT),
            P(None, "dp", EXPERT),
            P("section", "dp", EXPERT, None),
            P("section", "dp", EXPERT, None),
        ),
        out_specs=(
            P("section", None, "dp", EXPERT),
            P("section", None, "dp", EXPERT),
            P("section", "dp", EXPERT, None),
            P("section", "dp", EXPERT, None),
        ),
        check_vma=False,
    )
```

```python
import math

import jax
import jax.numpy as jnp
from jax import lax
from jax.experimental import pallas as pl
from jax.experimental.pallas import tpu as pltpu
from jax.sharding import Mesh
from jax.sharding import PartitionSpec as P

D = 2048
FF = 7168
EXPERTS = 4
EXPERT = ("z", "core")
BF = jnp.bfloat16
F32 = jnp.float32
CHUNKS = 16
LANES = 128
ROWS = 32
TOKS = EXPERTS * ROWS
HID = 224

NT = (((1,), (1,)), ((), ()))
TN = (((0,), (0,)), ((), ()))


VMEM, HBM, SMEM = pltpu.VMEM, pltpu.HBM, pltpu.SMEM


def call(body, outs, args, scratch=(), limit=24):
    return pl.pallas_call(
        body,
        out_shape=tuple(
            pltpu.HBM(shape, dtype) if space == HBM else jax.ShapeDtypeStruct(shape, dtype)
            for shape, dtype, space in outs
        ),
        in_specs=[pl.BlockSpec(memory_space=space) for _, space in args],
        out_specs=tuple(pl.BlockSpec(memory_space=space) for _, _, space in outs),
        scratch_shapes=list(scratch),
        compiler_params=pltpu.CompilerParams(vmem_limit_bytes=limit * 1024 * 1024),
    )(*(pltpu.with_memory_space_constraint(a, HBM) if space == HBM else a for a, space in args))


def sems(number):
    return pltpu.SemaphoreType.DMA((number,))


def halves(first, own, other):
    return jnp.where(first, jnp.concatenate([own, other], -1), jnp.concatenate([other, own], -1))


def pack_body(core, *refs):
    count = (len(refs) - 3) // 2
    inputs, (send, keep), held, arrived = refs[:count], refs[count : count + 2], refs[count + 2 : -1], refs[-1]
    copies = [
        pltpu.make_async_copy(ref, to, arrived.at[n]) for n, (ref, to) in enumerate(zip(inputs, held))
    ]
    for c in copies:
        c.start()
    mine = pl.multiple_of(core[0] * ROWS, ROWS)
    others = pl.multiple_of((1 - core[0]) * ROWS, ROWS)
    at = 0
    for c, ref in zip(copies, held):
        c.wait()
        for n in range(ref.shape[0]):
            keep[at] = ref[n, pl.ds(mine, ROWS), :]
            send[at] = ref[n, pl.ds(others, ROWS), :]
            at += 1


def pack(core, arrays):
    count = sum(a.shape[0] for a in arrays)
    shape = (count, ROWS, 64)
    return call(
        pack_body,
        ((shape, BF, VMEM), (shape, BF, VMEM)),
        ((core, SMEM), *((a, HBM) for a in arrays)),
        scratch=(*(pltpu.VMEM(a.shape, BF) for a in arrays), sems(len(arrays))),
    )


def open_body(core, keep, got, out, first, fresh, arrived):
    lead = jnp.full((ROWS, LANES), core[0], jnp.int32) == 0
    for n in range(6):
        rows = halves(lead, keep[n].astype(F32), got[n].astype(F32)).astype(BF)
        if n < 4:
            first[n * ROWS : (n + 1) * ROWS, :] = rows
        else:
            fresh[(n - 4) * ROWS : (n - 3) * ROWS, :] = rows
    copies = [pltpu.make_async_copy(first, out.at[k], arrived.at[k]) for k in range(CHUNKS)]
    for c in copies:
        c.start()
    for c in copies:
        c.wait()


def opened(core, keep, got):
    return call(
        open_body,
        (
            ((CHUNKS, 4 * ROWS, LANES), BF, HBM),
            ((4 * ROWS, LANES), BF, VMEM),
            ((2 * ROWS, LANES), BF, VMEM),
        ),
        ((core, SMEM), (keep, VMEM), (got, VMEM)),
        scratch=(sems(CHUNKS),),
    )


def next_body(place, arriving, leaving, fresh, out, second, arrived):
    at_first = jnp.full((ROWS, LANES), place[0], jnp.int32) == 0
    at_last = jnp.full((ROWS, LANES), place[1], jnp.int32) == 0
    second[0:ROWS, :] = jnp.where(at_first, fresh[0:ROWS, :].astype(F32), arriving[...].astype(F32)).astype(BF)
    second[ROWS : 2 * ROWS, :] = jnp.where(
        at_last, fresh[ROWS : 2 * ROWS, :].astype(F32), leaving[...].astype(F32)
    ).astype(BF)
    copies = [pltpu.make_async_copy(second, out.at[k], arrived.at[k]) for k in range(CHUNKS)]
    for c in copies:
        c.start()
    for c in copies:
        c.wait()


def following(place, arriving, leaving, fresh):
    return call(
        next_body,
        (((CHUNKS, 2 * ROWS, LANES), BF, HBM), ((2 * ROWS, LANES), BF, VMEM)),
        ((place, SMEM), (arriving, VMEM), (leaving, VMEM), (fresh, VMEM)),
        scratch=(sems(CHUNKS),),
    )


def spread_body(got, weight, out, staged, sent):
    rows = got.shape[1]
    copies = []
    for e in range(EXPERTS):
        scale = weight[e]
        for k in range(CHUNKS):
            staged[e, k, 0:ROWS, :] = got[k, 0:ROWS, :]
            staged[e, k, ROWS : 2 * ROWS, :] = (scale * got[k, ROWS : 2 * ROWS, :].astype(F32)).astype(BF)
            if rows > 2 * ROWS:
                staged[e, k, 2 * ROWS : rows, :] = got[k, 2 * ROWS : rows, :]
        copies.append(pltpu.make_async_copy(staged.at[e], out.at[e], sent.at[e]))
        copies[-1].start()
    for c in copies:
        c.wait()


def spread(got, weight):
    shape = (EXPERTS, *got.shape)
    return call(
        spread_body,
        ((shape, BF, HBM),),
        ((got, VMEM), (weight, VMEM)),
        scratch=(pltpu.VMEM(shape, BF), sems(EXPERTS)),
    )[0]


def layer_body(kept_at, came, *refs):
    refs = list(refs)
    kept = refs.pop(0) if kept_at is not None else None
    gate_own, gate_other, down_own, down_other, out, own, other = refs[:7]
    both, grad, staged, g_own, g_other, d_own, d_other, sent, loaded = refs[7:16]
    loads = [
        pltpu.make_async_copy(s, d, loaded.at[n])
        for n, (s, d) in enumerate(
            ((gate_own, g_own), (down_own, d_own), (gate_other, g_other), (down_other, d_other))
        )
    ]
    if kept_at is not None:
        stored = refs[16]
        loads.append(
            pltpu.make_async_copy(kept.at[:, :, pl.ds(kept_at, ROWS), :], stored, loaded.at[4])
        )
        loads[4].start()
    for c in loads[0:4]:
        c.start()
    for e in range(EXPERTS):
        for k in range(CHUNKS):
            lanes = slice(k * LANES, (k + 1) * LANES)
            both[e * ROWS : (e + 1) * ROWS, lanes] = came[e, k, 0:ROWS, :]
            grad[e * ROWS : (e + 1) * ROWS, lanes] = came[e, k, ROWS : 2 * ROWS, :]
            if kept_at is None:
                both[TOKS + e * ROWS : TOKS + (e + 1) * ROWS, lanes] = came[e, k, 2 * ROWS : 3 * ROWS, :]
    if kept_at is not None:
        loads[4].wait()
        for e in range(EXPERTS):
            for k in range(CHUNKS):
                lanes = slice(k * LANES, (k + 1) * LANES)
                both[TOKS + e * ROWS : TOKS + (e + 1) * ROWS, lanes] = stored[e, k]
    tokens, cotangent = both[...], grad[...]
    hidden_fwd, slopes = [], []
    for n, (gate, down, keep) in enumerate(((g_own, d_own, own), (g_other, d_other, other))):
        loads[2 * n].wait()
        before = lax.dot_general(tokens, gate[...], NT, preferred_element_type=F32)
        sigmoid = 1.0 / (1.0 + jnp.exp(-before))
        hidden = (before * sigmoid).astype(BF)
        hidden_fwd.append(hidden[0:TOKS])
        loads[2 * n + 1].wait()
        through = lax.dot_general(cotangent, down[...], NT, preferred_element_type=F32)
        sig, pre = sigmoid[TOKS:], before[TOKS:]
        slope = (through * sig * (1.0 + pre * (1.0 - sig))).astype(BF)
        slopes.append(slope)
        keep[0] = hidden[TOKS:]
        keep[1] = slope
    forward = jnp.dot(hidden_fwd[0], d_own[...], preferred_element_type=F32) + jnp.dot(
        hidden_fwd[1], d_other[...], preferred_element_type=F32
    )
    backward = jnp.dot(slopes[0], g_own[...], preferred_element_type=F32) + jnp.dot(
        slopes[1], g_other[...], preferred_element_type=F32
    )
    forward, backward = forward.astype(BF), backward.astype(BF)
    stores = []
    for e in range(EXPERTS):
        for k in range(CHUNKS):
            rows, lanes = slice(e * ROWS, (e + 1) * ROWS), slice(k * LANES, (k + 1) * LANES)
            staged[e, k, 0:ROWS, :] = forward[rows, lanes]
            staged[e, k, ROWS : 2 * ROWS, :] = backward[rows, lanes]
        stores.append(pltpu.make_async_copy(staged.at[e], out.at[e], sent.at[e]))
        stores[-1].start()
    for c in stores:
        c.wait()


def layer(came, kept, kept_at, weights):
    def body(*refs):
        layer_body(kept_at, *refs)

    shape = (EXPERTS, CHUNKS, 2 * ROWS, LANES)
    pair = (2, TOKS, HID)
    weight = pltpu.VMEM((HID, D), BF)
    scratch = [
        pltpu.VMEM((2 * TOKS, D), BF),
        pltpu.VMEM((TOKS, D), BF),
        pltpu.VMEM(shape, BF),
        *([weight] * 4),
        sems(EXPERTS),
        sems(5),
    ]
    args = [(came, VMEM)]
    if kept_at is not None:
        scratch.append(pltpu.VMEM((EXPERTS, CHUNKS, ROWS, LANES), BF))
        args.append((kept, HBM))
    return call(
        body,
        ((shape, BF, HBM), (pair, BF, VMEM), (pair, BF, VMEM)),
        (*args, *((w, HBM) for w in weights)),
        scratch=scratch,
    )


def combine_chunks(back, weight, out):
    for k in range(CHUNKS):
        fwd = weight[0] * back[0, k, 0:ROWS, :].astype(F32)
        bwd = back[0, k, ROWS : 2 * ROWS, :].astype(F32)
        for e in range(1, EXPERTS):
            fwd = fwd + weight[e] * back[e, k, 0:ROWS, :].astype(F32)
            bwd = bwd + back[e, k, ROWS : 2 * ROWS, :].astype(F32)
        out[k, 0:ROWS, :] = fwd.astype(BF)
        out[k, ROWS : 2 * ROWS, :] = bwd.astype(BF)


def combine_body(back, weight, out, staged, sent):
    combine_chunks(back, weight, staged)
    c = pltpu.make_async_copy(staged, out, sent.at[0])
    c.start()
    c.wait()


def combine_sum_body(back, weight, squares, out, staged, sent):
    combine_chunks(back, weight, staged)
    total = jnp.full((16, LANES), jnp.sum(squares[...]), F32)
    high = total.astype(BF).astype(F32)
    middle = (total - high).astype(BF).astype(F32)
    low = total - high - middle
    row = lax.broadcasted_iota(jnp.int32, (16, LANES), 0)
    zero = jnp.zeros((16, LANES), F32)
    pieces = jnp.where(row == 0, high, jnp.where(row == 1, middle, jnp.where(row == 2, low, zero))).astype(BF)
    for k in range(CHUNKS):
        staged[k, 2 * ROWS : 2 * ROWS + 16, :] = pieces
    c = pltpu.make_async_copy(staged, out, sent.at[0])
    c.start()
    c.wait()


def combine(back, weight, squares=None):
    shape = (CHUNKS, 2 * ROWS + (16 if squares is not None else 0), LANES)
    args = [(back, VMEM), (weight, VMEM)]
    if squares is not None:
        args.append((squares, VMEM))
    return call(
        combine_body if squares is None else combine_sum_body,
        ((shape, BF, HBM),),
        args,
        scratch=(pltpu.VMEM(shape, BF), sems(1)),
    )[0]


def grads_body(
    came0, came0p, came1, came1p, own0, own0p, own1, own1p, gate, down, squares,
    buf0, buf0p, buf1, buf1p, cot, stored, gate_v, down_v, loaded, sent,
):
    tail = pl.ds(ROWS, 3 * ROWS)
    one = pl.ds(ROWS, ROWS)
    loads = [
        pltpu.make_async_copy(came0.at[:, :, tail, :], buf0, loaded.at[0]),
        pltpu.make_async_copy(came0p.at[:, :, tail, :], buf0p, loaded.at[1]),
        pltpu.make_async_copy(came1.at[:, :, one, :], buf1, loaded.at[2]),
        pltpu.make_async_copy(came1p.at[:, :, one, :], buf1p, loaded.at[3]),
    ]
    for c in loads:
        c.start()
    sources = ((buf0, buf0, 1), (buf0p, buf0p, 1), (buf1, buf0, 2), (buf1p, buf0p, 2))
    for n, (came, kept, at) in enumerate(sources):
        loads[n].wait()
        for e in range(EXPERTS):
            for k in range(CHUNKS):
                rows = slice(n * TOKS + e * ROWS, n * TOKS + (e + 1) * ROWS)
                lanes = slice(k * LANES, (k + 1) * LANES)
                cot[rows, lanes] = came[e, k, 0:ROWS, :]
                stored[rows, lanes] = kept[e, k, at * ROWS : (at + 1) * ROWS, :]
    pairs = (own0, own0p, own1, own1p)
    hidden = jnp.concatenate([p[0] for p in pairs], axis=0)
    slope = jnp.concatenate([p[1] for p in pairs], axis=0)
    total = jnp.zeros((8, LANES), F32)
    width = 512
    stores = []
    for n, at in enumerate(range(0, D, width)):
        lanes = slice(at, at + width)
        for m, (left, right, out, held) in enumerate(
            ((slope, stored, gate, gate_v), (hidden, cot, down, down_v))
        ):
            part = lax.dot_general(left, right[:, lanes], TN, preferred_element_type=F32)
            held[:, lanes] = part
            stores.append(
                pltpu.make_async_copy(
                    held.at[:, pl.ds(at, width)], out.at[:, pl.ds(at, width)], sent.at[2 * n + m]
                )
            )
            stores[-1].start()
            square = jnp.sum((part * part).reshape(HID // 8, 8, width), axis=0)
            for lane in range(0, width, LANES):
                total = total + square[:, lane : lane + LANES]
    squares[...] = total
    for c in stores:
        c.wait()


def grads(cames, owns):
    tokens = 4 * TOKS
    total = ((HID, D), F32, HBM)
    return call(
        grads_body,
        (total, total, ((8, LANES), F32, VMEM)),
        (*((c, HBM) for c in cames), *((o, VMEM) for o in owns)),
        scratch=(
            pltpu.VMEM((EXPERTS, CHUNKS, 3 * ROWS, LANES), BF),
            pltpu.VMEM((EXPERTS, CHUNKS, 3 * ROWS, LANES), BF),
            pltpu.VMEM((EXPERTS, CHUNKS, ROWS, LANES), BF),
            pltpu.VMEM((EXPERTS, CHUNKS, ROWS, LANES), BF),
            pltpu.VMEM((tokens, D), BF),
            pltpu.VMEM((tokens, D), BF),
            pltpu.VMEM((HID, D), F32),
            pltpu.VMEM((HID, D), F32),
            sems(4),
            sems(8),
        ),
    )


def close_body(pieces, base, result, tiles):
    total = base[...].astype(F32)
    extra = jnp.zeros((16, LANES), F32)
    for k in range(CHUNKS):
        total = total + pieces[k, 0 : 2 * ROWS, :].astype(F32)
        extra = extra + pieces[k, 2 * ROWS : 2 * ROWS + 16, :].astype(F32)
    result[...] = total.astype(BF)
    along = jnp.sum(extra, axis=0, keepdims=True)
    for k in range(tiles.shape[0]):
        tiles[k] = jnp.broadcast_to(along, (8, LANES))


def closed(pieces, base, count):
    return call(
        close_body,
        (((2 * ROWS, LANES), BF, VMEM), ((count, 8, LANES), F32, VMEM)),
        ((pieces, VMEM), (base, VMEM)),
    )


STEP = 32


def clip_body(limit, tiles, gate, down, gate_out, down_out, gate_v, down_v, gate_o, down_o, loaded, sent):
    work = [
        (held, kept, out, pl.ds(at, STEP), pltpu.make_async_copy(
            source.at[pl.ds(at, STEP)], held.at[pl.ds(at, STEP)], loaded.at[m * (HID // STEP) + n]
        ))
        for n, at in enumerate(range(0, HID, STEP))
        for m, (source, held, kept, out) in enumerate(
            ((gate, gate_v, gate_o, gate_out), (down, down_v, down_o, down_out))
        )
    ]
    for *_, c in work:
        c.start()
    total = jnp.sum(tiles[...], axis=0)
    factor = (limit / jnp.maximum(jnp.sqrt(total), limit))[0:1, 0:1]
    stores = []
    for n, (held, kept, out, rows, c) in enumerate(work):
        c.wait()
        kept[rows, :] = (held[rows, :] * factor).astype(BF)
        stores.append(pltpu.make_async_copy(kept.at[rows], out.at[rows], sent.at[n]))
        stores[-1].start()
    for c in stores:
        c.wait()


def clipped(limit, tiles, gate, down):
    def body(*refs):
        clip_body(limit, *refs)

    number = 2 * (HID // STEP)
    out = ((HID, D), BF, HBM)
    return call(
        body,
        (out, out),
        ((tiles, VMEM), (gate, HBM), (down, HBM)),
        scratch=(
            pltpu.VMEM((HID, D), F32),
            pltpu.VMEM((HID, D), F32),
            pltpu.VMEM((HID, D), BF),
            pltpu.VMEM((HID, D), BF),
            sems(number),
            sems(number),
        ),
    )


def swapped(value):
    return lax.ppermute(value, "core", [(0, 1), (1, 0)])


def exchanged(value, axis):
    return lax.all_to_all(value, axis, 0, 0, tiled=True)


def shifted(value, steps):
    count = lax.axis_size("section")
    return lax.ppermute(
        value, "section", [(s, s + steps) for s in range(max(0, -steps), min(count, count - steps))]
    )


def lanes_home(result, first):
    rows = result.reshape(2, ROWS, 2, 64)
    low, high = rows[:, :, 0], rows[:, :, 1]
    got = swapped(jnp.where(first, high, low))
    mine = jnp.where(first, low, high)
    return jnp.where(first, jnp.concatenate([mine, got], 1), jnp.concatenate([got, mine], 1))


def gate_rows(experts, gate_values):
    half = lax.axis_index("core") * ROWS
    experts = lax.dynamic_slice_in_dim(experts, half, ROWS, 1)
    gate_values = lax.dynamic_slice_in_dim(gate_values, half, ROWS, 1)
    number = jnp.arange(EXPERTS, dtype=jnp.int32)[None, :, None, None]
    rows = jnp.sum(jnp.where(experts[:, None] == number, gate_values[:, None], F32(0.0)), axis=-1)
    return jnp.broadcast_to(rows[..., None], (*rows.shape, LANES))


def on_device(
    fwd_input,
    fresh_input,
    fwd_experts,
    fwd_gates,
    bwd_saved,
    bwd_experts,
    bwd_gates,
    out_grad,
    fresh_grad,
    gate_proj,
    down_proj,
):
    gate_own, down_own = gate_proj[0, 0], down_proj[0, 0]
    section_count = lax.axis_size("section")
    section_index = lax.axis_index("section")

    core_index = lax.axis_index("core").astype(jnp.int32)
    core = core_index[None]
    place = jnp.stack([section_index, section_count - 1 - section_index]).astype(jnp.int32)

    send, keep = pack(core, (fwd_input, out_grad, bwd_saved[0], fresh_input, fresh_grad))
    outgoing, first, fresh = opened(core, keep, swapped(send))

    weights = (gate_own, swapped(gate_own), down_own, swapped(down_own))
    fwd_weight = gate_rows(fwd_experts[0], fwd_gates[0])
    bwd_weight = gate_rows(bwd_experts[0], bwd_gates[0])

    got = exchanged(outgoing, "z")
    came0 = exchanged(spread(got, bwd_weight[0]), "dp")
    partial, own0, other0 = layer(came0, None, None, weights)
    came0, partial = lax.optimization_barrier((came0, partial))
    came0p, own0p = swapped(came0), swapped(other0)
    back = exchanged(partial, "dp")
    pieces = exchanged(combine(back, fwd_weight[0]), "z")
    base = first[0 : 2 * ROWS]
    result0 = (base.astype(F32) + jnp.sum(pieces.astype(F32), axis=0)).astype(BF)

    arriving = shifted(result0[0:ROWS], 1)
    leaving = shifted(result0[ROWS : 2 * ROWS], -1)
    outgoing, second = following(place, arriving, leaving, fresh)

    got = exchanged(outgoing, "z")
    came1 = exchanged(spread(got, bwd_weight[1]), "dp")
    partial, own1, other1 = layer(came1, came0, 3 * ROWS, weights)
    came1, partial = lax.optimization_barrier((came1, partial))
    came1p, own1p = swapped(came1), swapped(other1)
    back = exchanged(partial, "dp")
    gate_total, down_total, squares = grads(
        (came0, came0p, came1, came1p), (own0, own0p, own1, own1p)
    )
    pieces = exchanged(combine(back, fwd_weight[1], squares), "z")

    result1, tiles = closed(pieces, second, 32)
    tiles = exchanged(tiles, ("section", "dp", "core"))
    clip_limit = 0.25 * math.sqrt(2.0 * section_count * EXPERTS * FF * D)
    gate_grad, down_grad = clipped(clip_limit, tiles, gate_total, down_total)

    leads = core_index == 0
    home0, home1 = lanes_home(result0, leads), lanes_home(result1, leads)
    fwd_output = jnp.stack([home0[0], home1[0]])[None]
    input_grad = jnp.stack([home0[1], home1[1]])[None]
    return (fwd_output, input_grad, gate_grad[None, None], down_grad[None, None])


def solution(mesh):
    split = Mesh(
        mesh.devices.reshape(mesh.shape["section"], CHUNKS, 2, mesh.shape["dp"]),
        ("section", "z", "core", "dp"),
    )
    return jax.shard_map(
        on_device,
        mesh=split,
        in_specs=(
            P("section", "dp", EXPERT),
            P(None, "dp", EXPERT),
            P("section", None, "dp", None),
            P("section", None, "dp", None),
            P("section", None, "dp", EXPERT),
            P("section", None, "dp", None),
            P("section", None, "dp", None),
            P("section", "dp", EXPERT),
            P(None, "dp", EXPERT),
            P("section", "dp", EXPERT, None),
            P("section", "dp", EXPERT, None),
        ),
        out_specs=(
            P("section", None, "dp", EXPERT),
            P("section", None, "dp", EXPERT),
            P("section", "dp", EXPERT, None),
            P("section", "dp", EXPERT, None),
        ),
        check_vma=False,
    )
```
